128 devices in a mesh: dom: 16 (over y, z), shard: 8 (over x, core).
Axes of the slice: x: 4, y: 4, z: 4, core: 2. Of those that a mesh axis runs over, the one named last changes fastest.
Arguments:
- node_features: bfloat16 [65536, 768], P(('dom', 'shard')), may hold values from -6 to 6
- input_boundary: bfloat16 [262144, 768], P(('dom', 'shard')), may hold values from -6 to 6
- hidden_stale: bfloat16 [262144, 1024], P(('dom', 'shard')), may hold values from -4 to 4
- grad_stale: bfloat16 [65536, 1024], P(('dom', 'shard')), may hold values from -4 to 4
- cotangent: bfloat16 [65536, 1024], P(('dom', 'shard')), may hold values from -6 to 6
- weight_one: bfloat16 [768, 1024], replicated, may hold values from -0.21875 to 0.21875
- weight_two: bfloat16 [1024, 1024], replicated, may hold values from -0.1875 to 0.1875
- tile_values: bfloat16 [4096, 128, 128], P(('dom', 'shard')), may hold values from -0.1875 to 0.1875
- tile_list: int32 [4096, 3], P(('dom', 'shard')), may hold values from 0 to 31, as said below
- tile_count: int32 [128], P(('dom', 'shard')), may hold values from 16 to 32, as said below
- read_blocks: int32 [128, 16], P(('dom', 'shard')), may hold values from -1 to 3, as said below
Outputs:
- layer_out: bfloat16 [65536, 1024], P(('dom', 'shard'))
- hidden_fresh: bfloat16 [262144, 1024], P(('dom', 'shard'))
- grad_fresh: bfloat16 [65536, 1024], P(('dom', 'shard'))
- weight_grad_one: float32 [768, 1024], P('shard')
- weight_grad_two: float32 [1024, 1024], P('shard')
The draws below stay inside these ranges and needn't reach their ends.
Inputs may be any that keep to these rules, and one draw needn't show every extreme that they name: `read_blocks`: entry (p, k + c) names a row block of the partition that slot k + c of p stands for, or -1. The blocks that one partition reads from one other are distinct; a partition reads nothing from its own domain, and at most 1 block from each other domain. `tile_list`: row p * 32 + t gives tile t of partition p in three columns. Column 0 is its row block, 0 to 3. Column 1 is its column, 0 to 19: below 4 an own row block, else slot column - 4, never an empty slot. Column 2 is its tile id, 0 to 31; the ids of one partition are a permutation of 0 to 31. Tiles t with t >= tile_count[p] are not used.
All inputs are finite; a program needn't handle non-finite values.
Results may differ from the reference program's by a relative error of at most 0.0057.
Values may be sent and summed in bfloat16 or wider, within the bound.
No kernel may reach another device: no remote copies, remote signals or barrier semaphores. Data moves between devices by JAX's collectives and lax.ppermute only.
A program may use at most 128 MiB of HBM per device.

```python
import math
import jax
import jax.numpy as jnp
from jax import lax

BLOCK = 128
ROWS = 512
FEAT = 768
HID = 1024
NT = 32
CAP = 1
RB = 4
DOMAINS = 16
SLOTS = 16
PARTS_SIZE = 128
TOTAL_ROWS = 65536


def graph_layout(key):
    domains = SLOTS // CAP
    shards = PARTS_SIZE // domains
    keys = jax.random.split(jax.random.fold_in(key, 7), 5)
    present = jax.random.randint(keys[0], (PARTS_SIZE, domains, CAP), 0, 5) < 3
    scores = jax.random.randint(keys[1], (PARTS_SIZE, domains, RB), 0, 1 << 20) * RB + jnp.arange(RB)[None, None, :]
    ordering = jnp.argsort(scores, axis=-1, stable=True)[:, :, :CAP].astype(jnp.int32)
    home = jnp.arange(PARTS_SIZE) // shards
    forced = jnp.arange(domains)[None, :] == (home[:, None] + 1) % domains
    same = jnp.arange(domains)[None, :] == home[:, None]
    live = (present | forced[:, :, None]) & jnp.logical_not(same[:, :, None])
    reads = jnp.where(live, ordering, -1).reshape(PARTS_SIZE, SLOTS).astype(jnp.int32)
    columns_live = jnp.concatenate([jnp.ones((PARTS_SIZE, RB), jnp.int32), (reads >= 0).astype(jnp.int32)], axis=1)
    running = jnp.cumsum(columns_live, axis=1)
    totals = running[:, -1]
    picks = jax.random.randint(keys[2], (PARTS_SIZE, NT), 0, 1 << 20) % totals[:, None]
    tile_cols = jnp.sum((running[:, None, :] <= picks[:, :, None]).astype(jnp.int32), axis=2)
    tile_rows = jax.random.randint(keys[3], (PARTS_SIZE, NT), 0, RB)
    id_scores = jax.random.randint(keys[4], (PARTS_SIZE, NT), 0, 1 << 20) * NT + jnp.arange(NT)[None, :]
    tile_ids = jnp.argsort(id_scores, axis=-1, stable=True).astype(jnp.int32)
    listing = jnp.stack([tile_rows, tile_cols, tile_ids], axis=-1).astype(jnp.int32).reshape(PARTS_SIZE * NT, 3)
    return (reads, listing)


def draw_read_blocks(key, part):
    reads, listing = graph_layout(key)
    return reads


def draw_tile_list(key, part):
    reads, listing = graph_layout(key)
    return listing


def draw_tile_count(key, part):
    keys = jax.random.split(jax.random.fold_in(key, 11), 2)
    counts = jax.random.randint(keys[0], (PARTS_SIZE,), NT // 2, NT + 1)
    fullest = jax.random.randint(keys[1], (), 0, PARTS_SIZE)
    return jnp.where(jnp.arange(PARTS_SIZE) == fullest, NT, counts).astype(jnp.int32)


def levels(own_key, shape, cuts, low, top_value):
    level, own = 1.0, jax.random.fold_in(own_key, 6)
    for dim, blocks in cuts:
        heights = jnp.exp(jax.random.uniform(jax.random.fold_in(own, dim), (blocks,), jnp.float32, low / len(cuts), top_value / len(cuts)))
        level = level * jnp.repeat(heights, shape[dim] // blocks).reshape([-1 if axis == dim else 1 for axis in range(len(shape))])
    return level


def gaussian(key, extent, deviation, reach, pieces=(), dtype=jnp.bfloat16):
    loudness = levels(key, extent, pieces, -0.22, 0.18) if pieces else 1.0
    drawn = jax.random.normal(key, extent, jnp.float32) * deviation * loudness
    return jnp.minimum(jnp.maximum(drawn, -reach), reach).astype(dtype)


def setup_inputs(seed: int = 0) -> dict:
    key_list = jax.random.split(jax.random.key(seed), 12)
    return {
        "node_features": gaussian(key_list[0], (TOTAL_ROWS, FEAT), 1.0, 6.0, ((0, 128),)),
        "input_boundary": gaussian(key_list[1], (PARTS_SIZE * SLOTS * BLOCK, FEAT), 1.0, 6.0, ((0, 128),)),
        "hidden_stale": gaussian(key_list[2], (PARTS_SIZE * SLOTS * BLOCK, HID), 0.5, 4.0, ((0, 128),)),
        "grad_stale": gaussian(key_list[3], (TOTAL_ROWS, HID), 0.5, 4.0, ((0, 128),)),
        "cotangent": gaussian(key_list[4], (TOTAL_ROWS, HID), 1.0, 6.0, ((0, 128),)),
        "weight_one": gaussian(key_list[5], (FEAT, HID), FEAT ** -0.5, 0.21875),
        "weight_two": gaussian(key_list[6], (HID, HID), HID ** -0.5, 0.1875),
        "tile_values": gaussian(key_list[7], (PARTS_SIZE * NT, BLOCK, BLOCK), (BLOCK * NT // RB) ** -0.5, 0.1875, ((0, 128),)),
        "tile_list": draw_tile_list(jax.random.fold_in(key_list[11], 71), 0),
        "tile_count": draw_tile_count(jax.random.fold_in(key_list[11], 71), 0),
        "read_blocks": draw_read_blocks(jax.random.fold_in(key_list[11], 71), 0),
    }


def silu_slope(preact):
    sigmas = jax.nn.sigmoid(preact)
    return sigmas * (1.0 + preact * (1.0 - sigmas))

def combine_tiles(selected, tile_rows, tile_cols, live_tiles, source, row_blocks):
    picked = source[tile_cols].astype(jnp.float32)
    product = jnp.einsum('tij,tjw->tiw', selected.astype(jnp.float32), picked)
    row_table = ((jnp.arange(row_blocks)[:, None] == tile_rows[None, :]) & live_tiles[None, :]).astype(jnp.float32)
    summed = jnp.einsum('rt,tiw->riw', row_table, product, precision=lax.Precision.HIGHEST)
    return summed.reshape(row_blocks * source.shape[1], source.shape[2])

def spread_tiles(selected, tile_rows, tile_cols, live_tiles, grad_blocks, columns):
    picked = grad_blocks[tile_rows].astype(jnp.float32)
    product = jnp.einsum('tji,tjw->tiw', selected.astype(jnp.float32), picked)
    col_table = ((jnp.arange(columns)[:, None] == tile_cols[None, :]) & live_tiles[None, :]).astype(jnp.float32)
    return jnp.einsum('ct,tiw->ciw', col_table, product, precision=lax.Precision.HIGHEST)

def reference(node_features, input_boundary, hidden_stale, grad_stale, cotangent, weight_one, weight_two, tile_values, tile_list, tile_count, read_blocks):
    row_blocks = ROWS // BLOCK
    shards = PARTS_SIZE // DOMAINS
    feat_all = node_features.reshape(PARTS_SIZE, row_blocks, BLOCK, FEAT)
    bound_all = input_boundary.reshape(PARTS_SIZE, SLOTS, BLOCK, FEAT)
    tiles_all = tile_values.reshape(PARTS_SIZE, NT, BLOCK, BLOCK)
    lists_all = tile_list.reshape(PARTS_SIZE, NT, 3)

    def first_layer(inputs):
        feat_here, bound_here, tiles_here, list_here, count_here = inputs
        selected = tiles_here[list_here[:, 2]]
        live_tiles = jnp.arange(NT) < count_here
        source = jnp.concatenate([feat_here, bound_here], axis=0)
        pooled = combine_tiles(selected, list_here[:, 0], list_here[:, 1], live_tiles, source, row_blocks).astype(jnp.bfloat16)
        preact = jnp.dot(pooled, weight_one, preferred_element_type=jnp.float32)
        hidden = jax.nn.silu(preact).astype(jnp.bfloat16)
        return (pooled, preact, hidden)
    pooled_all, preact_all, hidden_all = lax.map(first_layer, (feat_all, bound_all, tiles_all, lists_all, tile_count))
    hidden_blocks = hidden_all.reshape(PARTS_SIZE * row_blocks, BLOCK, HID)
    reader = jnp.arange(PARTS_SIZE)[:, None]
    sender = (jnp.arange(SLOTS) // CAP)[None, :] * shards + reader % shards
    source_index = (sender * row_blocks + jnp.maximum(read_blocks, 0)).astype(jnp.int32)
    live_slots = (read_blocks >= 0)[:, :, None, None]
    fresh = jnp.where(live_slots, hidden_blocks[source_index], jnp.zeros((), jnp.bfloat16))
    hidden_fresh = fresh.reshape(PARTS_SIZE * SLOTS * BLOCK, HID)
    stale_all = hidden_stale.reshape(PARTS_SIZE, SLOTS, BLOCK, HID)
    cot_all = cotangent.reshape(PARTS_SIZE, ROWS, HID)
    gstale_all = grad_stale.reshape(PARTS_SIZE, ROWS, HID)

    def second_layer(carry, inputs):
        hidden_here, stale_here, tiles_here, list_here, count_here, pooled, preact, cot_here, gstale_here = inputs
        selected = tiles_here[list_here[:, 2]]
        live_tiles = jnp.arange(NT) < count_here
        source = jnp.concatenate([hidden_here.reshape(row_blocks, BLOCK, HID), stale_here], axis=0)
        mixed = combine_tiles(selected, list_here[:, 0], list_here[:, 1], live_tiles, source, row_blocks).astype(jnp.bfloat16)
        output = jnp.dot(mixed, weight_two, preferred_element_type=jnp.float32).astype(jnp.bfloat16)
        grad_mixed = jnp.dot(cot_here, weight_two.T, preferred_element_type=jnp.float32).astype(jnp.bfloat16)
        back_sums = spread_tiles(selected, list_here[:, 0], list_here[:, 1], live_tiles, grad_mixed.reshape(row_blocks, BLOCK, HID), row_blocks + SLOTS)
        grad_hidden = back_sums[:row_blocks].reshape(ROWS, HID) + gstale_here.astype(jnp.float32)
        grad_pre = (grad_hidden * silu_slope(preact)).astype(jnp.bfloat16)
        returns = back_sums[row_blocks:].astype(jnp.bfloat16)
        sum_one = carry[0] + jnp.dot(pooled.T, grad_pre, preferred_element_type=jnp.float32)
        sum_two = carry[1] + jnp.dot(mixed.T, cot_here, preferred_element_type=jnp.float32)
        return ((sum_one, sum_two), (output, returns))
    start = (jnp.zeros((FEAT, HID), jnp.float32), jnp.zeros((HID, HID), jnp.float32))
    inputs = (hidden_all, stale_all, tiles_all, lists_all, tile_count, pooled_all, preact_all, cot_all, gstale_all)
    (sum_one, sum_two), (outputs, returns) = lax.scan(second_layer, start, inputs)
    layer_out = outputs.reshape(PARTS_SIZE * ROWS, HID)
    contributions = jnp.where(live_slots, returns.astype(jnp.float32), jnp.zeros((), jnp.float32))
    collected = jnp.zeros((PARTS_SIZE * row_blocks, BLOCK, HID), jnp.float32)
    collected = collected.at[source_index.reshape(-1)].add(contributions.reshape(PARTS_SIZE * SLOTS, BLOCK, HID))
    grad_fresh = collected.astype(jnp.bfloat16).reshape(PARTS_SIZE * ROWS, HID)
    grad_scale = 1.0 / math.sqrt(TOTAL_ROWS)
    return (layer_out, hidden_fresh, grad_fresh, sum_one * grad_scale, sum_two * grad_scale)
```

```python
import math

import jax
import jax.numpy as jnp
from jax import lax
from jax.experimental import pallas as pl
from jax.experimental.pallas import tpu as pltpu
from jax.sharding import Mesh
from jax.sharding import PartitionSpec as P

DOM = ("dom_0", "dom_1")
DOM_SHARD = ("dom_0", "dom_1", "shard")
BF16 = jnp.bfloat16
F32 = jnp.float32
VMEM_LIMIT = 60 * 1024 * 1024


def dot_f32(a, b, dims):
    return lax.dot_general(a, b, (dims, ((), ())), preferred_element_type=F32)


def started(copies):
    for copy in copies:
        copy.start()
    return copies


def finished(copies):
    for copy in copies:
        copy.wait()


def cut_copies(source, target, sems, first, pieces):
    length = source.shape[0] // pieces
    return [
        pltpu.make_async_copy(
            source.at[pl.ds(k * length, length)], target.at[pl.ds(k * length, length)], sems.at[first + k]
        )
        for k in range(pieces)
    ]


def backward_kernel(
    row_blocks, list_ref, count_ref, tiles_hbm, cot_hbm, weight_hbm,
    adj_hbm, returns_hbm, own_hbm,
    tiles, cot, weight, adj, dense, grad_mixed, returns, own, in_sems, out_sems,
):
    size = tiles.shape[1]
    groups, _, _ = adj.shape
    tile_copies = started(cut_copies(tiles_hbm, tiles, in_sems, 0, 4))
    cot_copies = started(cut_copies(cot_hbm, cot, in_sems, 4, 2))
    weight_copies = started(cut_copies(weight_hbm, weight, in_sems, 6, 4))
    dense[...] = jnp.zeros_like(dense)
    count = count_ref[0]
    finished(tile_copies)

    def add_tile(t, carry):
        row, column, tile = list_ref[0, t], list_ref[1, t], list_ref[2, t]
        group = column // row_blocks
        inside = column - group * row_blocks
        place = (
            group,
            pl.ds(pl.multiple_of(row * size, size), size),
            pl.ds(pl.multiple_of(inside * size, size), size),
        )
        value = tiles[tile].astype(F32)
        dense[place] += jnp.where(t < count, value, jnp.zeros_like(value))
        return carry

    lax.fori_loop(0, tiles.shape[0], add_tile, 0, unroll=4)
    finished(cot_copies)
    finished(weight_copies)
    grad_mixed[...] = dot_f32(cot[...], weight[...], ((1,), (1,))).astype(BF16)
    out_copies = []
    for k in range(groups):
        group = (k + 1) % groups
        adj[group] = dense[group].astype(BF16)
        sums = dot_f32(adj[group], grad_mixed[...], ((0,), (0,)))
        if group:
            returns[group - 1] = sums.astype(BF16)
            source, target = returns.at[group - 1], returns_hbm.at[group - 1]
        else:
            own[...] = sums
            source, target = own, own_hbm
        out_copies += started(cut_copies(source, target, out_sems, 4 * k, 2))
        out_copies += started(cut_copies(adj.at[group], adj_hbm.at[group], out_sems, 4 * k + 2, 1))
    finished(out_copies)


def anywhere(count):
    return [pl.BlockSpec(memory_space=pl.ANY)] * count


def backward_sums(tile_list, tile_count, tiles, cotangent, weight_two, row_blocks, slots):
    rows, width = cotangent.shape
    groups = (row_blocks + slots) // row_blocks
    flops = 2 * rows * width * (width + groups * rows)
    return pl.pallas_call(
        lambda *refs: backward_kernel(row_blocks, *refs),
        in_specs=[pl.BlockSpec(memory_space=pltpu.SMEM)] * 2 + anywhere(3),
        out_specs=anywhere(3),
        scratch_shapes=[
            pltpu.VMEM(tiles.shape, BF16),
            pltpu.VMEM(cotangent.shape, BF16),
            pltpu.VMEM(weight_two.shape, BF16),
            pltpu.VMEM((groups, rows, rows), BF16),
            pltpu.VMEM((groups, rows, rows), F32),
            pltpu.VMEM((rows, width), BF16),
            pltpu.VMEM((groups - 1, rows, width), BF16),
            pltpu.VMEM((rows, width), F32),
            pltpu.SemaphoreType.DMA((10,)),
            pltpu.SemaphoreType.DMA((4 * groups,)),
        ],
        out_shape=[
            jax.ShapeDtypeStruct((groups, rows, rows), BF16),
            jax.ShapeDtypeStruct((groups - 1, rows, width), BF16),
            jax.ShapeDtypeStruct((rows, width), F32),
        ],
        compiler_params=pltpu.CompilerParams(vmem_limit_bytes=VMEM_LIMIT),
        cost_estimate=pl.CostEstimate(flops=flops, bytes_accessed=14 * 2**20, transcendentals=0),
        name="backward_sums",
    )(tile_list.T, tile_count, tiles, cotangent, weight_two)


def forward_kernel(
    scale, shards,
    core_ref, adj_hbm, feat_hbm, bound_hbm, one_hbm, stale_hbm, cot_hbm, own_hbm, gstale_hbm,
    hidden_hbm, mixed_hbm, kept_hbm, sent_hbm,
    adj, source, one, hidden_all, cot, own, gstale, pooled, grad_pre, mixed, weights, in_sems, out_sems,
):
    groups, rows, _ = adj_hbm.shape
    width = one.shape[1]
    step = 256
    adj_copies = started([
        pltpu.make_async_copy(adj_hbm.at[g], adj.at[:, pl.ds(g * rows, rows)], in_sems.at[g])
        for g in range(groups)
    ])
    base = groups
    front = started(cut_copies(feat_hbm, source.at[pl.ds(0, rows)], in_sems, base, 1))
    front += started(cut_copies(bound_hbm, source.at[pl.ds(rows, bound_hbm.shape[0])], in_sems, base + 1, 4))
    one_copies = started(cut_copies(one_hbm, one, in_sems, base + 5, 2))
    own_copies = started(cut_copies(own_hbm, own, in_sems, base + 7, 2))
    own_copies += started(cut_copies(gstale_hbm, gstale, in_sems, base + 9, 1))
    stale_copies = started(
        cut_copies(stale_hbm, hidden_all.at[pl.ds(rows, stale_hbm.shape[0])], in_sems, base + 10, 4)
    )
    cot_copies = started(cut_copies(cot_hbm, cot, in_sems, base + 14, 1))
    finished(adj_copies)
    finished(front)
    matrix = ((1,), (0,))
    for c in range(0, source.shape[1], step):
        cols = pl.ds(c, step)
        pooled[:, cols] = dot_f32(adj[...], source[:, cols], matrix).astype(BF16)
    finished(one_copies)
    finished(own_copies)
    for c in range(0, width, step):
        cols = pl.ds(c, step)
        preact = dot_f32(pooled[...], one[:, cols], matrix)
        sigmas = 1.0 / (1.0 + jnp.exp(-preact))
        hidden_all[pl.ds(0, rows), cols] = (preact * sigmas).astype(BF16)
        slope = sigmas * (1.0 + preact * (1.0 - sigmas))
        grad_pre[:, cols] = ((own[:, cols] + gstale[:, cols].astype(F32)) * slope).astype(BF16)
    out_copies = started(cut_copies(hidden_all.at[pl.ds(0, rows)], hidden_hbm, out_sems, 0, 2))
    finished(stale_copies)
    for c in range(0, width, step):
        cols = pl.ds(c, step)
        mixed[:, cols] = dot_f32(adj[...], hidden_all[:, cols], matrix).astype(BF16)
    out_copies += started(cut_copies(mixed, mixed_hbm, out_sems, 2, 2))
    finished(cot_copies)
    across = ((0,), (0,))
    one_rows, two_rows = pooled.shape[1] // shards, width // shards
    both = one_rows + two_rows
    place = [(s % 2 * (shards // 2) + s // 2) * both for s in range(shards)]
    for c in range(0, width, step):
        cols = pl.ds(c, step)
        first = dot_f32(pooled[...], grad_pre[:, cols], across) * scale
        for s in range(shards):
            weights[pl.ds(place[s], one_rows), cols] = first[s * one_rows : (s + 1) * one_rows]
        second = dot_f32(mixed[...], cot[:, cols], across) * scale
        for s in range(shards):
            weights[pl.ds(place[s] + one_rows, two_rows), cols] = second[s * two_rows : (s + 1) * two_rows]
    half = shards // 2 * both
    mine = core_ref[0]
    for k, (target, which) in enumerate(((sent_hbm, 1 - mine), (kept_hbm, mine))):
        source = weights.at[pl.ds(pl.multiple_of(which * half, half), half)]
        out_copies += started(cut_copies(source, target, out_sems, 4 + 4 * k, 4))
    finished(out_copies)


def forward_sums(core, adj, features, boundary, weight_one, stale, cotangent, own, grad_stale, scale, shards):
    rows, feat = features.shape
    width = weight_one.shape[1]
    columns = rows + boundary.shape[0]
    flops = 2 * rows * (columns * (feat + width) + 2 * feat * width + width * width)
    return pl.pallas_call(
        lambda *refs: forward_kernel(scale, shards, *refs),
        in_specs=[pl.BlockSpec(memory_space=pltpu.SMEM)] + anywhere(8),
        out_specs=anywhere(4),
        scratch_shapes=[
            pltpu.VMEM((rows, columns), BF16),
            pltpu.VMEM((columns, feat), BF16),
            pltpu.VMEM(weight_one.shape, BF16),
            pltpu.VMEM((columns, width), BF16),
            pltpu.VMEM((rows, width), BF16),
            pltpu.VMEM((rows, width), F32),
            pltpu.VMEM((rows, width), BF16),
            pltpu.VMEM((rows, feat), BF16),
            pltpu.VMEM((rows, width), BF16),
            pltpu.VMEM((rows, width), BF16),
            pltpu.VMEM((feat + width, width), F32),
            pltpu.SemaphoreType.DMA((adj.shape[0] + 15,)),
            pltpu.SemaphoreType.DMA((12,)),
        ],
        out_shape=[
            jax.ShapeDtypeStruct((rows, width), BF16),
            jax.ShapeDtypeStruct((rows, width), BF16),
            jax.ShapeDtypeStruct(((feat + width) // 2, width), F32),
            jax.ShapeDtypeStruct(((feat + width) // 2, width), F32),
        ],
        compiler_params=pltpu.CompilerParams(vmem_limit_bytes=VMEM_LIMIT),
        cost_estimate=pl.CostEstimate(flops=flops, bytes_accessed=26 * 2**20, transcendentals=0),
        name="forward_sums",
    )(core, adj, features, boundary, weight_one, stale, cotangent, own, grad_stale)


def pack_kernel(wanted_ref, blocks_hbm, out_hbm, held, in_sems, out_sems):
    count, size, _ = blocks_hbm.shape
    copies = started([
        pltpu.make_async_copy(blocks_hbm.at[k], held.at[k], in_sems.at[k]) for k in range(count)
    ])
    held[count] = jnp.zeros(held.shape[1:], held.dtype)
    finished(copies)
    out_copies = []
    for reader in range(out_hbm.shape[0]):
        want = wanted_ref[reader]
        source = held.at[jnp.where(want < 0, count, want)]
        target = out_hbm.at[reader, pl.ds(0, size)]
        out_copies.append(pltpu.make_async_copy(source, target, out_sems.at[reader]))
    finished(started(out_copies))


def packed_blocks(wanted, blocks, extra):
    readers = wanted.shape[0]
    count, size, width = blocks.shape
    return pl.pallas_call(
        pack_kernel,
        in_specs=[pl.BlockSpec(memory_space=pltpu.SMEM)] + anywhere(1),
        out_specs=anywhere(1)[0],
        scratch_shapes=[
            pltpu.VMEM((count + 1, size, width), BF16),
            pltpu.SemaphoreType.DMA((count,)),
            pltpu.SemaphoreType.DMA((readers,)),
        ],
        out_shape=jax.ShapeDtypeStruct((readers, size + extra, width), BF16),
        compiler_params=pltpu.CompilerParams(vmem_limit_bytes=VMEM_LIMIT),
        cost_estimate=pl.CostEstimate(flops=4 * 10**9, bytes_accessed=5 * 2**20, transcendentals=0),
        name="pack_blocks",
    )(wanted, blocks)


def append_kernel(rows_hbm, packed_hbm, out_hbm, held, in_sem, out_sems):
    readers, extra, _ = rows_hbm.shape
    size = out_hbm.shape[1] - extra
    finished(started([pltpu.make_async_copy(rows_hbm, held, in_sem)]))
    finished(started([
        pltpu.make_async_copy(held.at[k], out_hbm.at[k, pl.ds(size, extra)], out_sems.at[k])
        for k in range(readers)
    ]))


def with_rows(packed, rows):
    return pl.pallas_call(
        append_kernel,
        in_specs=anywhere(2),
        out_specs=anywhere(1)[0],
        scratch_shapes=[
            pltpu.VMEM(rows.shape, BF16),
            pltpu.SemaphoreType.DMA,
            pltpu.SemaphoreType.DMA((rows.shape[0],)),
        ],
        out_shape=jax.ShapeDtypeStruct(packed.shape, BF16),
        input_output_aliases={1: 0},
        compiler_params=pltpu.CompilerParams(vmem_limit_bytes=VMEM_LIMIT),
        cost_estimate=pl.CostEstimate(flops=10**9, bytes_accessed=2**20, transcendentals=0),
        name="append_rows",
    )(rows, packed)


def collect_kernel(wanted_ref, in_ref, out_ref, total):
    reader = pl.program_id(0)

    @pl.when(reader == 0)
    def _():
        total[...] = jnp.zeros_like(total)

    want = wanted_ref[reader]

    @pl.when(want >= 0)
    def _():
        total[want] += in_ref[0].astype(F32)

    @pl.when(reader == pl.num_programs(0) - 1)
    def _():
        out_ref[...] = total[...].astype(BF16)


def collected_blocks(wanted, arrived, row_blocks):
    readers, size, width = arrived.shape
    return pl.pallas_call(
        collect_kernel,
        grid_spec=pltpu.PrefetchScalarGridSpec(
            num_scalar_prefetch=1,
            grid=(readers,),
            in_specs=[pl.BlockSpec((1, size, width), lambda i, w: (i, 0, 0))],
            out_specs=pl.BlockSpec((row_blocks, size, width), lambda i, w: (0, 0, 0)),
            scratch_shapes=[pltpu.VMEM((row_blocks, size, width), F32)],
        ),
        out_shape=jax.ShapeDtypeStruct((row_blocks, size, width), BF16),
        compiler_params=pltpu.CompilerParams(dimension_semantics=("arbitrary",)),
        cost_estimate=pl.CostEstimate(flops=4 * 10**9, bytes_accessed=5 * 2**20, transcendentals=0),
        name="collect_blocks",
    )(wanted, arrived)


def shifted(array, axis, by):
    count = lax.axis_size(axis)
    return lax.ppermute(array, axis, [(i, (i + by) % count) for i in range(count)])


def scattered_sum(parts, axis, stride, wire):
    count = parts(0)[1]
    own = parts(0)[0]
    got = [shifted(parts(k)[0].astype(wire), axis, k * stride) for k in range(1, count)]
    for value in got:
        own = own + value.astype(F32)
    return own


def shard_share(kept, sent, wire):
    shards = lax.axis_size("shard")
    chips = shards // 2
    chip = lax.axis_index("shard") // 2
    other = lax.ppermute(sent, "shard", [(i, i ^ 1) for i in range(shards)])
    rows, width = kept.shape[0] // chips, kept.shape[1]
    kept, other = kept.reshape(chips, rows, width), other.reshape(chips, rows, width)

    def chip_part(k):
        at = lax.rem(chip + k, chips)
        pick = lambda a: lax.dynamic_index_in_dim(a, at, 0, keepdims=False)
        return pick(kept) + pick(other), chips

    return scattered_sum(chip_part, "shard", 2, wire)


def exchanged(parts):
    return lax.all_to_all(parts, DOM, split_axis=0, concat_axis=0, tiled=True)


def wanted_blocks(read_blocks):
    tiles = jnp.broadcast_to(read_blocks.reshape(-1, 1, 1), (read_blocks.size, 8, 128))
    return exchanged(tiles)[:, 0, 0]


def local(
    node_features,
    input_boundary,
    hidden_stale,
    grad_stale,
    cotangent,
    weight_one,
    weight_two,
    tile_values,
    tile_list,
    tile_count,
    read_blocks,
):
    size = tile_values.shape[1]
    row_count = node_features.shape[0]
    row_blocks = row_count // size
    slots = read_blocks.shape[1]
    width = weight_one.shape[1]

    parts = lax.axis_size(DOM) * lax.axis_size("shard")
    scale = 1.0 / math.sqrt(row_count * parts)
    core = (lax.axis_index("shard") % 2).reshape(1)
    wanted = wanted_blocks(read_blocks)
    adj, returns, own = backward_sums(
        tile_list, tile_count, tile_values, cotangent, weight_two, row_blocks, slots
    )
    wanted, returns = lax.optimization_barrier((wanted, returns))
    arrived = exchanged(returns.reshape(slots, size, width))
    hidden, mixed, kept, sent = forward_sums(
        core, adj, node_features, input_boundary, weight_one, hidden_stale, cotangent, own,
        grad_stale, scale, lax.axis_size("shard"),
    )
    share = shard_share(kept, sent, BF16)
    share_rows = share.shape[0] // slots
    extra = -(-share_rows // 16) * 16
    packed = packed_blocks(wanted, hidden.reshape(row_blocks, size, width), extra)
    rows = share.astype(BF16).reshape(slots, share_rows, width)
    rows = jnp.pad(rows, ((0, 0), (0, extra - share_rows), (0, 0)))
    outgoing = with_rows(packed, rows)
    outgoing, arrived = lax.optimization_barrier((outgoing, arrived))
    fresh = exchanged(outgoing)
    grad_fresh = collected_blocks(wanted, arrived, row_blocks).reshape(row_count, width)
    layer_out = dot_f32(mixed, weight_two, ((1,), (0,))).astype(BF16)
    total = fresh[:, size:].astype(F32).sum(0).astype(BF16)
    totals = exchanged(jnp.broadcast_to(total[None], (slots, *total.shape)))
    hidden_fresh = fresh[:, :size].reshape(slots * size, width)
    sums = totals[:, :share_rows].reshape(-1, width).astype(F32)
    cut = weight_one.shape[0] // lax.axis_size("shard")
    return (layer_out, hidden_fresh, grad_fresh, sums[:cut], sums[cut:])


def solution(mesh):
    torus = Mesh(mesh.devices.reshape(4, 4, mesh.shape["shard"]), ("dom_0", "dom_1", "shard"))

    return jax.shard_map(
        local,
        mesh=torus,
        in_specs=(
            P(DOM_SHARD, None),
            P(DOM_SHARD, None),
            P(DOM_SHARD, None),
            P(DOM_SHARD, None),
            P(DOM_SHARD, None),
            P(),
            P(),
            P(DOM_SHARD, None, None),
            P(DOM_SHARD, None),
            P(DOM_SHARD),
            P(DOM_SHARD, None),
        ),
        out_specs=(
            P(DOM_SHARD, None),
            P(DOM_SHARD, None),
            P(DOM_SHARD, None),
            P("shard", None),
            P("shard", None),
        ),
        check_vma=False,
    )
```

```python
import math

import jax
import jax.numpy as jnp
from jax import lax
from jax.experimental import pallas as pl
from jax.experimental.pallas import tpu as pltpu
from jax.sharding import Mesh
from jax.sharding import PartitionSpec as P

DOM = ("dom_0", "dom_1")
DOM_SHARD = ("dom_0", "dom_1", "shard")
SHIFT_GROUPS = (
    ((0, 3), (0, 1), (3, 0), (1, 0)),
    ((0, 2), (2, 0), (3, 1)),
    ((1, 3), (3, 3), (1, 1)),
    ((3, 2), (2, 3)),
    ((2, 1), (1, 2), (2, 2)),
)
SHIFTS = sum(SHIFT_GROUPS, ())
BF16 = jnp.bfloat16
F32 = jnp.float32
VMEM_LIMIT = 60 * 1024 * 1024


def dot_f32(a, b, dims):
    return lax.dot_general(a, b, (dims, ((), ())), preferred_element_type=F32)


def started(copies):
    for copy in copies:
        copy.start()
    return copies


def finished(copies):
    for copy in copies:
        copy.wait()


def cut_copies(source, target, sems, first, pieces):
    length = source.shape[0] // pieces
    return [
        pltpu.make_async_copy(
            source.at[pl.ds(k * length, length)], target.at[pl.ds(k * length, length)], sems.at[first + k]
        )
        for k in range(pieces)
    ]


def backward_kernel(
    row_blocks, list_ref, count_ref, tiles_hbm, cot_hbm, weight_hbm,
    adj_hbm, returns_hbm, own_hbm,
    tiles, cot, weight, adj, dense, grad_mixed, returns, own, in_sems, out_sems,
):
    size = tiles.shape[1]
    groups, _, _ = adj.shape
    tile_copies = started(cut_copies(tiles_hbm, tiles, in_sems, 0, 4))
    cot_copies = started(cut_copies(cot_hbm, cot, in_sems, 4, 2))
    weight_copies = started(cut_copies(weight_hbm, weight, in_sems, 6, 4))
    dense[...] = jnp.zeros_like(dense)
    count = count_ref[0]
    finished(tile_copies)

    def add_tile(t, carry):
        row, column, tile = list_ref[0, t], list_ref[1, t], list_ref[2, t]
        group = column // row_blocks
        inside = column - group * row_blocks
        place = (
            group,
            pl.ds(pl.multiple_of(row * size, size), size),
            pl.ds(pl.multiple_of(inside * size, size), size),
        )
        value = tiles[tile].astype(F32)
        dense[place] += jnp.where(t < count, value, jnp.zeros_like(value))
        return carry

    lax.fori_loop(0, tiles.shape[0], add_tile, 0, unroll=4)
    finished(cot_copies)
    finished(weight_copies)
    grad_mixed[...] = dot_f32(cot[...], weight[...], ((1,), (1,))).astype(BF16)
    out_copies = []
    for k in range(groups):
        group = (k + 1) % groups
        adj[group] = dense[group].astype(BF16)
        sums = dot_f32(adj[group], grad_mixed[...], ((0,), (0,)))
        if group:
            returns[group - 1] = sums.astype(BF16)
            source, target = returns.at[group - 1], returns_hbm.at[group - 1]
        else:
            own[...] = sums
            source, target = own, own_hbm
        out_copies += started(cut_copies(source, target, out_sems, 4 * k, 2))
        out_copies += started(cut_copies(adj.at[group], adj_hbm.at[group], out_sems, 4 * k + 2, 1))
    finished(out_copies)


def anywhere(count):
    return [pl.BlockSpec(memory_space=pl.ANY)] * count


def backward_sums(tile_list, tile_count, tiles, cotangent, weight_two, row_blocks, slots):
    rows, width = cotangent.shape
    groups = (row_blocks + slots) // row_blocks
    flops = 2 * rows * width * (width + groups * rows)
    return pl.pallas_call(
        lambda *refs: backward_kernel(row_blocks, *refs),
        in_specs=[pl.BlockSpec(memory_space=pltpu.SMEM)] * 2 + anywhere(3),
        out_specs=anywhere(3),
        scratch_shapes=[
            pltpu.VMEM(tiles.shape, BF16),
            pltpu.VMEM(cotangent.shape, BF16),
            pltpu.VMEM(weight_two.shape, BF16),
            pltpu.VMEM((groups, rows, rows), BF16),
            pltpu.VMEM((groups, rows, rows), F32),
            pltpu.VMEM((rows, width), BF16),
            pltpu.VMEM((groups - 1, rows, width), BF16),
            pltpu.VMEM((rows, width), F32),
            pltpu.SemaphoreType.DMA((10,)),
            pltpu.SemaphoreType.DMA((4 * groups,)),
        ],
        out_shape=[
            jax.ShapeDtypeStruct((groups, rows, rows), BF16),
            jax.ShapeDtypeStruct((groups - 1, rows, width), BF16),
            jax.ShapeDtypeStruct((rows, width), F32),
        ],
        compiler_params=pltpu.CompilerParams(vmem_limit_bytes=VMEM_LIMIT),
        cost_estimate=pl.CostEstimate(flops=flops, bytes_accessed=14 * 2**20, transcendentals=0),
        name="backward_sums",
    )(tile_list.T, tile_count, tiles, cotangent, weight_two)


def forward_kernel(
    scale, shards,
    core_ref, adj_hbm, feat_hbm, bound_hbm, one_hbm, stale_hbm, cot_hbm, own_hbm, gstale_hbm,
    hidden_hbm, mixed_hbm, kept_hbm, sent_hbm,
    adj, source, one, hidden_all, cot, own, gstale, pooled, grad_pre, mixed, weights, in_sems, out_sems,
):
    groups, rows, _ = adj_hbm.shape
    width = one.shape[1]
    step = 256
    adj_copies = started([
        pltpu.make_async_copy(adj_hbm.at[g], adj.at[:, pl.ds(g * rows, rows)], in_sems.at[g])
        for g in range(groups)
    ])
    base = groups
    front = started(cut_copies(feat_hbm, source.at[pl.ds(0, rows)], in_sems, base, 1))
    front += started(cut_copies(bound_hbm, source.at[pl.ds(rows, bound_hbm.shape[0])], in_sems, base + 1, 4))
    one_copies = started(cut_copies(one_hbm, one, in_sems, base + 5, 2))
    own_copies = started(cut_copies(own_hbm, own, in_sems, base + 7, 2))
    own_copies += started(cut_copies(gstale_hbm, gstale, in_sems, base + 9, 1))
    stale_copies = started(
        cut_copies(stale_hbm, hidden_all.at[pl.ds(rows, stale_hbm.shape[0])], in_sems, base + 10, 4)
    )
    cot_copies = started(cut_copies(cot_hbm, cot, in_sems, base + 14, 1))
    finished(adj_copies)
    finished(front)
    matrix = ((1,), (0,))
    for c in range(0, source.shape[1], step):
        cols = pl.ds(c, step)
        pooled[:, cols] = dot_f32(adj[...], source[:, cols], matrix).astype(BF16)
    finished(one_copies)
    finished(own_copies)
    for c in range(0, width, step):
        cols = pl.ds(c, step)
        preact = dot_f32(pooled[...], one[:, cols], matrix)
        sigmas = 1.0 / (1.0 + jnp.exp(-preact))
        hidden_all[pl.ds(0, rows), cols] = (preact * sigmas).astype(BF16)
        slope = sigmas * (1.0 + preact * (1.0 - sigmas))
        grad_pre[:, cols] = ((own[:, cols] + gstale[:, cols].astype(F32)) * slope).astype(BF16)
    out_copies = started(cut_copies(hidden_all.at[pl.ds(0, rows)], hidden_hbm, out_sems, 0, 2))
    finished(stale_copies)
    for c in range(0, width, step):
        cols = pl.ds(c, step)
        mixed[:, cols] = dot_f32(adj[...], hidden_all[:, cols], matrix).astype(BF16)
    out_copies += started(cut_copies(mixed, mixed_hbm, out_sems, 2, 2))
    finished(cot_copies)
    across = ((0,), (0,))
    one_rows, two_rows = pooled.shape[1] // shards, width // shards
    both = one_rows + two_rows
    place = [(s % 2 * (shards // 2) + s // 2) * both for s in range(shards)]
    for c in range(0, width, step):
        cols = pl.ds(c, step)
        first = dot_f32(pooled[...], grad_pre[:, cols], across) * scale
        for s in range(shards):
            weights[pl.ds(place[s], one_rows), cols] = first[s * one_rows : (s + 1) * one_rows]
        second = dot_f32(mixed[...], cot[:, cols], across) * scale
        for s in range(shards):
            weights[pl.ds(place[s] + one_rows, two_rows), cols] = second[s * two_rows : (s + 1) * two_rows]
    half = shards // 2 * both
    mine = core_ref[0]
    for k, (target, which) in enumerate(((sent_hbm, 1 - mine), (kept_hbm, mine))):
        source = weights.at[pl.ds(pl.multiple_of(which * half, half), half)]
        out_copies += started(cut_copies(source, target, out_sems, 4 + 4 * k, 4))
    finished(out_copies)


def forward_sums(core, adj, features, boundary, weight_one, stale, cotangent, own, grad_stale, scale, shards):
    rows, feat = features.shape
    width = weight_one.shape[1]
    columns = rows + boundary.shape[0]
    flops = 2 * rows * (columns * (feat + width) + 2 * feat * width + width * width)
    return pl.pallas_call(
        lambda *refs: forward_kernel(scale, shards, *refs),
        in_specs=[pl.BlockSpec(memory_space=pltpu.SMEM)] + anywhere(8),
        out_specs=anywhere(4),
        scratch_shapes=[
            pltpu.VMEM((rows, columns), BF16),
            pltpu.VMEM((columns, feat), BF16),
            pltpu.VMEM(weight_one.shape, BF16),
            pltpu.VMEM((columns, width), BF16),
            pltpu.VMEM((rows, width), BF16),
            pltpu.VMEM((rows, width), F32),
            pltpu.VMEM((rows, width), BF16),
            pltpu.VMEM((rows, feat), BF16),
            pltpu.VMEM((rows, width), BF16),
            pltpu.VMEM((rows, width), BF16),
            pltpu.VMEM((feat + width, width), F32),
            pltpu.SemaphoreType.DMA((adj.shape[0] + 15,)),
            pltpu.SemaphoreType.DMA((12,)),
        ],
        out_shape=[
            jax.ShapeDtypeStruct((rows, width), BF16),
            jax.ShapeDtypeStruct((rows, width), BF16),
            jax.ShapeDtypeStruct(((feat + width) // 2, width), F32),
            jax.ShapeDtypeStruct(((feat + width) // 2, width), F32),
        ],
        compiler_params=pltpu.CompilerParams(vmem_limit_bytes=VMEM_LIMIT),
        cost_estimate=pl.CostEstimate(flops=flops, bytes_accessed=26 * 2**20, transcendentals=0),
        name="forward_sums",
    )(core, adj, features, boundary, weight_one, stale, cotangent, own, grad_stale)


def neighbour(place_ref, shift, sign):
    y = (place_ref[0] + sign * shift[0]) & 3
    return y * 4 + ((place_ref[1] + sign * shift[1]) & 3)


def pack_kernel(wanted_ref, place_ref, blocks_hbm, *rest):
    outs, (held, in_sems, out_sems) = rest[: len(SHIFTS)], rest[len(SHIFTS) :]
    count = blocks_hbm.shape[0]
    copies = started([
        pltpu.make_async_copy(blocks_hbm.at[k], held.at[k], in_sems.at[k]) for k in range(count)
    ])
    held[count] = jnp.zeros(held.shape[1:], held.dtype)
    finished(copies)
    out_copies = []
    for k, target in enumerate(outs):
        want = wanted_ref[neighbour(place_ref, SHIFTS[k], 1)]
        source = held.at[jnp.where(want < 0, count, want)]
        out_copies.append(pltpu.make_async_copy(source, target, out_sems.at[k]))
    finished(started(out_copies))


def packed_blocks(wanted, place, blocks):
    count, size, width = blocks.shape
    return pl.pallas_call(
        pack_kernel,
        in_specs=[pl.BlockSpec(memory_space=pltpu.SMEM)] * 2 + anywhere(1),
        out_specs=anywhere(len(SHIFTS)),
        scratch_shapes=[
            pltpu.VMEM((count + 1, size, width), BF16),
            pltpu.SemaphoreType.DMA((count,)),
            pltpu.SemaphoreType.DMA((len(SHIFTS),)),
        ],
        out_shape=[jax.ShapeDtypeStruct((size, width), BF16)] * len(SHIFTS),
        compiler_params=pltpu.CompilerParams(vmem_limit_bytes=VMEM_LIMIT),
        cost_estimate=pl.CostEstimate(flops=4 * 10**9, bytes_accessed=5 * 2**20, transcendentals=0),
        name="pack_blocks",
    )(wanted, place, blocks)


def place_kernel(place_ref, *rest):
    blocks, out_hbm = rest[: len(SHIFTS)], rest[len(SHIFTS)]
    held, in_sems, out_sems = rest[len(SHIFTS) + 1 :]
    copies = started([
        pltpu.make_async_copy(source, held.at[k], in_sems.at[k]) for k, source in enumerate(blocks)
    ])
    empty = len(SHIFTS)
    held[empty] = jnp.zeros(held.shape[1:], held.dtype)
    out_copies = started([
        pltpu.make_async_copy(held.at[empty], out_hbm.at[neighbour(place_ref, (0, 0), 1)], out_sems.at[empty])
    ])
    for k, copy in enumerate(copies):
        copy.wait()
        out_copies += started([
            pltpu.make_async_copy(held.at[k], out_hbm.at[neighbour(place_ref, SHIFTS[k], -1)], out_sems.at[k])
        ])
    finished(out_copies)


def placed_blocks(place, blocks):
    size, width = blocks[0].shape
    count = len(SHIFTS) + 1
    return pl.pallas_call(
        place_kernel,
        in_specs=[pl.BlockSpec(memory_space=pltpu.SMEM)] + anywhere(len(SHIFTS)),
        out_specs=anywhere(1)[0],
        scratch_shapes=[
            pltpu.VMEM((count, size, width), BF16),
            pltpu.SemaphoreType.DMA((len(SHIFTS),)),
            pltpu.SemaphoreType.DMA((count,)),
        ],
        out_shape=jax.ShapeDtypeStruct((count, size, width), BF16),
        compiler_params=pltpu.CompilerParams(vmem_limit_bytes=VMEM_LIMIT),
        cost_estimate=pl.CostEstimate(flops=4 * 10**9, bytes_accessed=8 * 2**20, transcendentals=0),
        name="place_blocks",
    )(place, *blocks)


def collect_kernel(wanted_ref, blocks_hbm, out_ref, held, total, sems):
    copies = started([
        pltpu.make_async_copy(blocks_hbm.at[k], held.at[k], sems.at[k])
        for k in range(blocks_hbm.shape[0])
    ])
    total[...] = jnp.zeros_like(total)
    for k, copy in enumerate(copies):
        copy.wait()
        want = wanted_ref[k]

        @pl.when(want >= 0)
        def _(k=k, want=want):
            total[want] += held[k].astype(F32)

    out_ref[...] = total[...].astype(BF16)


def collected_blocks(wanted, arrived, row_blocks):
    readers, size, width = arrived.shape
    return pl.pallas_call(
        collect_kernel,
        in_specs=[pl.BlockSpec(memory_space=pltpu.SMEM)] + anywhere(1),
        out_specs=pl.BlockSpec(memory_space=pltpu.VMEM),
        scratch_shapes=[
            pltpu.VMEM((readers, size, width), BF16),
            pltpu.VMEM((row_blocks, size, width), F32),
            pltpu.SemaphoreType.DMA((readers,)),
        ],
        out_shape=jax.ShapeDtypeStruct((row_blocks, size, width), BF16),
        compiler_params=pltpu.CompilerParams(vmem_limit_bytes=VMEM_LIMIT),
        cost_estimate=pl.CostEstimate(flops=4 * 10**9, bytes_accessed=5 * 2**20, transcendentals=0),
        name="collect_blocks",
    )(wanted, arrived)


def shifted(array, axis, by):
    count = lax.axis_size(axis)
    return lax.ppermute(array, axis, [(i, (i + by) % count) for i in range(count)])


def scattered_sum(parts, axis, stride, wire):
    count = parts(0)[1]
    own = parts(0)[0]
    got = [shifted(parts(k)[0].astype(wire), axis, k * stride) for k in range(1, count)]
    for value in got:
        own = own + value.astype(F32)
    return own


def shard_share(kept, sent, wire):
    shards = lax.axis_size("shard")
    chips = shards // 2
    chip = lax.axis_index("shard") // 2
    other = lax.ppermute(sent, "shard", [(i, i ^ 1) for i in range(shards)])
    rows, width = kept.shape[0] // chips, kept.shape[1]
    kept, other = kept.reshape(chips, rows, width), other.reshape(chips, rows, width)

    def chip_part(k):
        at = lax.rem(chip + k, chips)
        pick = lambda a: lax.dynamic_index_in_dim(a, at, 0, keepdims=False)
        return pick(kept) + pick(other), chips

    return scattered_sum(chip_part, "shard", 2, wire)


def exchanged(parts):
    return lax.all_to_all(parts, DOM, split_axis=0, concat_axis=0, tiled=True)


def wanted_blocks(read_blocks):
    tiles = jnp.broadcast_to(read_blocks.reshape(-1, 1, 1), (read_blocks.size, 8, 128))
    return exchanged(tiles)[:, 0, 0]


def gathered(part, axis):
    count, me = lax.axis_size(axis), lax.axis_index(axis)
    whole = jnp.zeros((count, *part.shape), part.dtype)
    for k in range(count):
        value = shifted(part, axis, k) if k else part
        whole = lax.dynamic_update_index_in_dim(whole, value, lax.rem(me - k + count, count), 0)
    return whole


def axis_parts(whole, axis):
    count, me = lax.axis_size(axis), lax.axis_index(axis)
    cut = whole.reshape(count, -1, 8, 128)

    def part(k):
        return lax.dynamic_index_in_dim(cut, lax.rem(me + k, count), 0, keepdims=False), count

    return part


def sent_by(array, shift):
    major, minor = (lax.axis_size(a) for a in DOM)
    pairs = [
        (y * minor + z, (y + shift[0]) % major * minor + (z + shift[1]) % minor)
        for y in range(major)
        for z in range(minor)
    ]
    return lax.ppermute(array, DOM, pairs)


def local(
    node_features,
    input_boundary,
    hidden_stale,
    grad_stale,
    cotangent,
    weight_one,
    weight_two,
    tile_values,
    tile_list,
    tile_count,
    read_blocks,
):
    size = tile_values.shape[1]
    row_count = node_features.shape[0]
    row_blocks = row_count // size
    slots = read_blocks.shape[1]
    width = weight_one.shape[1]

    parts = lax.axis_size(DOM) * lax.axis_size("shard")
    scale = 1.0 / math.sqrt(row_count * parts)
    core = (lax.axis_index("shard") % 2).reshape(1)
    wanted = wanted_blocks(read_blocks)
    adj, returns, own = backward_sums(
        tile_list, tile_count, tile_values, cotangent, weight_two, row_blocks, slots
    )
    wanted, returns = lax.optimization_barrier((wanted, returns))
    arrived = exchanged(returns.reshape(slots, size, width))
    hidden, mixed, kept, sent = forward_sums(
        core, adj, node_features, input_boundary, weight_one, hidden_stale, cotangent, own,
        grad_stale, scale, lax.axis_size("shard"),
    )
    place = jnp.stack([lax.axis_index(a) for a in DOM])
    share = shard_share(kept, sent, BF16)
    share_rows = share.shape[0]
    packed = packed_blocks(wanted, place, hidden.reshape(row_blocks, size, width))
    groups = []
    for group in SHIFT_GROUPS:
        at = sum(len(g) for g in groups)
        groups.append(packed[at : at + len(group)])
    fresh = []

    def send(k):
        fresh.extend(sent_by(block, shift) for block, shift in zip(groups[k], SHIFT_GROUPS[k]))

    send(0)
    tiles = share.reshape(share_rows // 8, 8, width // 128, 128).transpose(0, 2, 1, 3)
    part = scattered_sum(axis_parts(tiles.reshape(-1, 8, 128), DOM[0]), DOM[0], 1, BF16)
    send(1)
    part = scattered_sum(axis_parts(part, DOM[1]), DOM[1], 1, F32)
    send(2)
    part = gathered(part.astype(BF16), DOM[1]).reshape(-1, 8, 128)
    send(3)
    send(4)
    part = gathered(part, DOM[0]).reshape(-1, 8, 128)
    grad_fresh = collected_blocks(wanted, arrived, row_blocks).reshape(row_count, width)
    layer_out = dot_f32(mixed, weight_two, ((1,), (0,))).astype(BF16)
    sums = part.reshape(share_rows // 8, width // 128, 8, 128).transpose(0, 2, 1, 3)
    sums = sums.reshape(share_rows, width).astype(F32)
    hidden_fresh = placed_blocks(place, fresh).reshape(slots * size, width)
    cut = weight_one.shape[0] // lax.axis_size("shard")
    return (layer_out, hidden_fresh, grad_fresh, sums[:cut], sums[cut:])


def solution(mesh):
    torus = Mesh(mesh.devices.reshape(4, 4, mesh.shape["shard"]), ("dom_0", "dom_1", "shard"))

    return jax.shard_map(
        local,
        mesh=torus,
        in_specs=(
            P(DOM_SHARD, None),
            P(DOM_SHARD, None),
            P(DOM_SHARD, None),
            P(DOM_SHARD, None),
            P(DOM_SHARD, None),
            P(),
            P(),
            P(DOM_SHARD, None, None),
            P(DOM_SHARD, None),
            P(DOM_SHARD),
            P(DOM_SHARD, None),
        ),
        out_specs=(
            P(DOM_SHARD, None),
            P(DOM_SHARD, None),
            P(DOM_SHARD, None),
            P("shard", None),
            P("shard", None),
        ),
        check_vma=False,
    )
```
